32 devices in a mesh: cells: 32 (over z, y, x, core).
Axes of the slice: x: 2, y: 2, z: 4, core: 2. Of those that a mesh axis runs over, the one named last changes fastest.
Arguments:
- field: float32 [9, 55, 32768], P(None, None, 'cells'), may hold values from -6 to 6
- cell_area: float32 [32768], P('cells'), may hold values from 0.5 to 2
- dv_edge: float32 [103424], P('cells'), may hold values from 0.6 to 1.6
- dc_edge: float32 [103424], P('cells'), may hold values from 0.6 to 1.6
- cells_on_edge: int32 [2, 103424], P(None, 'cells'), may hold values from 0 to 1407, as said below
- edges_on_cell: int32 [6, 32768], P(None, 'cells'), may hold values from 0 to 3231, as said below
- send_cells: int32 [6, 2048], P(None, 'cells'), may hold values from 0 to 1023
- level_coef: float32 [55], replicated, may hold values from 0.005 to 0.02
Outputs:
- tendency: float32 [9, 55, 32768], P(None, None, 'cells')
The draws below stay inside these ranges and needn't reach their ends.
Inputs may be any that keep to these rules, and one draw needn't show every extreme that they name: `cells_on_edge`: the blocks tile one periodic hexagonal mesh, each a parallelogram of 64 by 16 cells; block b borders b + 1 and b - 1 along the first direction, b + 16 and b - 16 along the second, and b + 15 and b - 15 at one cell each, all modulo 32. Every edge with a cell in a block is listed once in that block, with the same dv_edge and dc_edge wherever it is listed, plus one extra entry that no cell names. Cells and edges are numbered in random order in each block. `edges_on_cell`: each cell names six distinct edges of its block.
All inputs are finite; a program needn't handle non-finite values.
Results may differ from the reference program's by a relative error of at most 0.00005.
Values sent between devices are 32-bit elements; how exact they have to be, the bound alone decides.
A program may use at most 128 MiB of HBM per device.

```python
import math
import jax
import jax.numpy as jnp
import numpy as np
from jax import lax

CELLS_X = 64
CELLS_Y = 16
FIELDS = 9
LEVELS = 55
BLOCK_ROW = 16
BLOCKS = 32
CELLS_DEV = 1024
SLOT = 64
EDGES_DEV = 3232
TOTAL_CELLS = 32768


def canonical_tables():
    width = CELLS_X
    height = CELLS_Y
    cell_count = width * height
    places = np.arange(cell_count)
    column = places % width
    row_index = places // width
    step_x = np.array([1, 0, 1])
    step_y = np.array([0, 1, -1])
    owned_dir = np.tile(np.arange(3), cell_count)
    owned_sx = np.repeat(column, 3)
    owned_sy = np.repeat(row_index, 3)
    owned_tx = owned_sx + step_x[owned_dir]
    owned_ty = owned_sy + step_y[owned_dir]
    along_y = np.arange(height)
    along_x = np.arange(width)
    short_x = np.arange(width - 1)
    src_x = np.concatenate([owned_sx, -np.ones(height, np.int64), -np.ones(height, np.int64), along_x, short_x, np.zeros(1, np.int64)])
    src_y = np.concatenate([owned_sy, along_y, along_y + 1, -np.ones(width, np.int64), height * np.ones(width - 1, np.int64), np.zeros(1, np.int64)])
    dst_x = np.concatenate([owned_tx, np.zeros(height, np.int64), np.zeros(height, np.int64), along_x, short_x + 1, np.zeros(1, np.int64)])
    dst_y = np.concatenate([owned_ty, along_y, along_y, np.zeros(width, np.int64), (height - 1) * np.ones(width - 1, np.int64), np.zeros(1, np.int64)])
    edge_dir = np.concatenate([owned_dir, np.zeros(height, np.int64), 2 * np.ones(height, np.int64), np.ones(width, np.int64), 2 * np.ones(width - 1, np.int64), np.zeros(1, np.int64)])
    base = 3 * cell_count
    beside_all = np.stack([places * 3, places * 3 + 1, places * 3 + 2, np.where(column > 0, (places - 1) * 3, base + row_index), np.where(row_index > 0, (places - width) * 3 + 1, base + 2 * height + column), np.where((column > 0) & (row_index < height - 1), (places + width - 1) * 3 + 2, np.where(column == 0, base + height + row_index, base + 2 * height + width + column - 1))])
    return (src_x, src_y, dst_x, dst_y, edge_dir, beside_all)


def frame_slots(coord_x, coord_y):
    width = CELLS_X
    height = CELLS_Y
    cell_count = width * height
    slot_len = CELLS_X
    inside_y = (coord_y >= 0) & (coord_y < height)
    inside_x = (coord_x >= 0) & (coord_x < width)
    is_own = inside_x & inside_y
    own_place = np.clip(coord_y, 0, height - 1) * width + np.clip(coord_x, 0, width - 1)
    halo_index = np.where((coord_x == -1) & inside_y, cell_count + coord_y, np.where((coord_x == width) & inside_y, cell_count + slot_len + coord_y, np.where((coord_y == -1) & inside_x, cell_count + 2 * slot_len + coord_x, np.where((coord_y == height) & inside_x, cell_count + 3 * slot_len + coord_x, np.where((coord_x == width) & (coord_y == -1), cell_count + 4 * slot_len + 0 * coord_x, np.where((coord_x == -1) & (coord_y == height), cell_count + 5 * slot_len + 0 * coord_x, 0))))))
    return (is_own, own_place, halo_index)


def mesh_numbering(key):
    cell_keys = jax.random.split(jax.random.fold_in(key, 11), BLOCKS)
    edge_keys = jax.random.split(jax.random.fold_in(key, 12), BLOCKS)
    place_of_cell = jax.vmap(lambda sub: jax.random.permutation(sub, CELLS_DEV))(cell_keys).astype(jnp.int32)
    cell_of_place = jnp.argsort(place_of_cell, axis=1).astype(jnp.int32)
    canon_of_edge = jax.vmap(lambda sub: jax.random.permutation(sub, EDGES_DEV))(edge_keys).astype(jnp.int32)
    edge_of_canon = jnp.argsort(canon_of_edge, axis=1).astype(jnp.int32)
    return (place_of_cell, cell_of_place, canon_of_edge, edge_of_canon)


def draw_cells_on_edge(key, part):
    src_x, src_y, dst_x, dst_y, edge_dir, beside_all = canonical_tables()
    place_of_cell, cell_of_place, canon_of_edge, edge_of_canon = mesh_numbering(key)
    results = []
    for coord_x, coord_y in ((src_x, src_y), (dst_x, dst_y)):
        is_own, own_place, halo_index = frame_slots(coord_x, coord_y)
        own_local = jnp.take(cell_of_place, jnp.asarray(own_place, jnp.int32), axis=1)
        canon_value = jnp.where(jnp.asarray(is_own)[None, :], own_local, jnp.asarray(halo_index, jnp.int32)[None, :])
        results.append(jnp.take_along_axis(canon_value, canon_of_edge, axis=1))
    return jnp.stack(results).reshape(2, BLOCKS * EDGES_DEV).astype(jnp.int32)


def draw_edges_on_cell(key, part):
    src_x, src_y, dst_x, dst_y, edge_dir, beside_all = canonical_tables()
    place_of_cell, cell_of_place, canon_of_edge, edge_of_canon = mesh_numbering(key)
    canon_edges = jnp.take(jnp.asarray(beside_all, jnp.int32), place_of_cell, axis=1)
    local_edges = jnp.take_along_axis(jnp.broadcast_to(edge_of_canon, (6, BLOCKS, EDGES_DEV)), canon_edges, axis=2)
    return local_edges.reshape(6, BLOCKS * CELLS_DEV).astype(jnp.int32)


def draw_send_cells(key, part):
    width = CELLS_X
    height = CELLS_Y
    place_of_cell, cell_of_place, canon_of_edge, edge_of_canon = mesh_numbering(key)
    entry = np.arange(CELLS_X)
    short = np.minimum(entry, height - 1)
    positions = np.stack([short * width + width - 1, short * width, (height - 1) * width + entry, entry, (height - 1) * width + 0 * entry, width - 1 + 0 * entry])
    limits = np.array([height, height, width, width, 1, 1])
    valid = entry[None, :] < limits[:, None]
    chosen = jnp.take(cell_of_place, jnp.asarray(positions, jnp.int32), axis=1)
    chosen = jnp.where(jnp.asarray(valid)[None, :, :], chosen, 0)
    return jnp.transpose(chosen, (1, 0, 2)).reshape(6, BLOCKS * SLOT).astype(jnp.int32)


def edge_global_ids(key):
    src_x, src_y, dst_x, dst_y, edge_dir, beside_all = canonical_tables()
    place_of_cell, cell_of_place, canon_of_edge, edge_of_canon = mesh_numbering(key)
    block_x = src_x // CELLS_X
    block_y = src_y // CELLS_Y
    src_place = src_y % CELLS_Y * CELLS_X + src_x % CELLS_X
    block_step = jnp.asarray(block_x + BLOCK_ROW * block_y, jnp.int32)
    block_ids = lax.broadcasted_iota(jnp.int32, (BLOCKS, EDGES_DEV), 0)
    owner = jnp.mod(block_ids + block_step[None, :], BLOCKS)
    global_ids = (owner * CELLS_DEV + jnp.asarray(src_place, jnp.int32)[None, :]) * 3 + jnp.asarray(edge_dir, jnp.int32)[None, :]
    return jnp.take_along_axis(global_ids, canon_of_edge, axis=1).reshape(BLOCKS * EDGES_DEV)


def draw_dv_edge(key, part):
    sub = jax.random.fold_in(key, 21)
    count = BLOCKS * CELLS_DEV * 3
    table = jnp.exp(jax.random.uniform(sub, (count,), jnp.float32, math.log(0.7), math.log(1.4)))
    return jnp.take(table, edge_global_ids(key)).astype(jnp.float32)


def draw_dc_edge(key, part):
    sub = jax.random.fold_in(key, 22)
    count = BLOCKS * CELLS_DEV * 3
    table = jnp.exp(jax.random.uniform(sub, (count,), jnp.float32, math.log(0.7), math.log(1.4)))
    return jnp.take(table, edge_global_ids(key)).astype(jnp.float32)


def level_of(stream_key, shape, cuts, least, high):
    level = 1.0
    for axis_at, blocks in cuts:
        steps = jax.random.uniform(jax.random.fold_in(jax.random.fold_in(stream_key, 6), axis_at), (blocks,), jnp.float32, least / len(cuts), high / len(cuts))
        level = level * jnp.repeat(jnp.exp(steps), shape[axis_at] // blocks).reshape((-1,) + (1,) * (len(shape) - 1 - axis_at))
    return level


def bell_draw(key, shape, scale, most, cuts=(), held_as=jnp.bfloat16):
    values = scale * jax.random.normal(key, shape, jnp.float32)
    if cuts:
        values = values * level_of(key, shape, cuts, -0.22, 0.18)
    return jnp.clip(values, -most, most).astype(held_as)


def setup_inputs(seed: int = 0) -> dict:
    arg_keys = jax.random.split(jax.random.key(seed), 9)
    field = bell_draw(arg_keys[0], (FIELDS, LEVELS, TOTAL_CELLS), 1.0, 6.0, ((2, 32),), jnp.float32)
    cell_area = jnp.clip(jnp.exp(math.log(2.0) - 1.3862944 * jax.random.uniform(arg_keys[1], (TOTAL_CELLS,), jnp.float32) ** level_of(arg_keys[1], (TOTAL_CELLS,), ((0, 32),), -0.2, 0.2)), 0.5, 2.0)
    dv_edge = draw_dv_edge(jax.random.fold_in(arg_keys[8], 71), 0)
    dc_edge = draw_dc_edge(jax.random.fold_in(arg_keys[8], 71), 0)
    cells_on_edge = draw_cells_on_edge(jax.random.fold_in(arg_keys[8], 71), 0)
    edges_on_cell = draw_edges_on_cell(jax.random.fold_in(arg_keys[8], 71), 0)
    send_cells = draw_send_cells(jax.random.fold_in(arg_keys[8], 71), 0)
    level_coef = jnp.clip(jnp.exp(jax.random.uniform(arg_keys[7], (LEVELS,), jnp.float32, math.log(0.005), math.log(0.02))), 0.005, 0.02)
    return {"field": field, "cell_area": cell_area, "dv_edge": dv_edge, "dc_edge": dc_edge, "cells_on_edge": cells_on_edge, "edges_on_cell": edges_on_cell, "send_cells": send_cells, "level_coef": level_coef}


def reference(field, cell_area, dv_edge, dc_edge, cells_on_edge, edges_on_cell, send_cells, level_coef):
    blocks = BLOCKS
    weight = (dv_edge / dc_edge).reshape(blocks, EDGES_DEV)
    area_block = cell_area.reshape(blocks, CELLS_DEV)
    endpoints = cells_on_edge.reshape(2, blocks, EDGES_DEV)
    beside_all = edges_on_cell.reshape(6, blocks, CELLS_DEV)
    send_lists = send_cells.reshape(6, blocks, SLOT)
    offsets = (1, -1, BLOCK_ROW, -BLOCK_ROW, BLOCK_ROW - 1, 1 - BLOCK_ROW)
    first_end = jnp.take_along_axis(jnp.broadcast_to(endpoints[0], (6, blocks, EDGES_DEV)), beside_all, axis=2)
    own_index = lax.broadcasted_iota(jnp.int32, (6, blocks, CELLS_DEV), 2)
    orient = jnp.where(first_end == own_index, 1.0, -1.0).astype(jnp.float32)

    def laplacian(values):
        pieces = [values]
        for direction in range(6):
            source = jnp.roll(values, offsets[direction], axis=0)
            chosen = jnp.roll(send_lists[direction], offsets[direction], axis=0)
            pieces.append(jnp.take_along_axis(source, chosen, axis=1))
        extended = jnp.concatenate(pieces, axis=1)
        upper_end = jnp.take_along_axis(extended, endpoints[1], axis=1)
        lower_end = jnp.take_along_axis(extended, endpoints[0], axis=1)
        fluxes = weight * (upper_end - lower_end)
        gathered = jnp.take_along_axis(jnp.broadcast_to(fluxes, (6, blocks, EDGES_DEV)), beside_all, axis=2)
        return jnp.sum(orient * gathered, axis=0) / area_block

    def one_level(packed):
        values, factor = packed
        return -factor * laplacian(laplacian(values))

    level_rows = field.reshape(FIELDS * LEVELS, blocks, CELLS_DEV)
    factors = jnp.tile(level_coef, FIELDS)
    result = lax.map(one_level, (level_rows, factors))
    return result.reshape(FIELDS, LEVELS, blocks * CELLS_DEV)
```

```python
import functools

import jax
import jax.numpy as jnp
from jax import lax
from jax.experimental import pallas as pl
from jax.experimental.pallas import tpu as pltpu
from jax.sharding import PartitionSpec as P

CELLS_Y = 16
BLOCK_ROW = 16
OFFSETS = (1, -1, BLOCK_ROW, -BLOCK_ROW, BLOCK_ROW - 1, 1 - BLOCK_ROW)
LANES = 128
CHUNKS = 2


def up(value, step):
    return -(-value // step) * step


def slots(length):
    side = CELLS_Y
    counts = (side, side, length, length, 8, 8)
    order = (2, 3, 0, 1, 4, 5)
    base = [0] * 6
    at = 0
    for k in order:
        base[k] = at
        at += counts[k]
    return tuple(base), counts, at


def prepare_kernel(
    dv_ref, dc_ref, ends_ref, edges_ref, send_ref, area_ref, near_ref, coef_ref, cols_ref,
    weight, packed, index,
):
    edge_count = dv_ref.shape[1]
    cell_count = edges_ref.shape[1]
    length = send_ref.shape[1]
    base, counts, _ = slots(length)
    tables = weight.shape[1] // LANES
    weight[...] = jnp.zeros_like(weight)
    packed[...] = jnp.zeros_like(packed)
    index[...] = jnp.zeros_like(index)
    weight[:, :edge_count] = dv_ref[...] / dc_ref[...]
    packed[:, :edge_count] = ends_ref[0:1, :] + ends_ref[1:2, :] * 4096
    index[0:6, :] = edges_ref[...]
    row = lax.broadcasted_iota(jnp.int32, (8, LANES), 0)
    lane = lax.broadcasted_iota(jnp.int32, (8, LANES), 1)
    for tile in range(cell_count // LANES):
        here = slice(tile * LANES, (tile + 1) * LANES)
        wanted = index[:, here]
        high = wanted >> 7
        low = wanted & 127
        w = jnp.zeros((8, LANES), jnp.float32)
        p = jnp.zeros((8, LANES), jnp.int32)
        for k in range(tables):
            part = slice(k * LANES, (k + 1) * LANES)
            wk = jnp.broadcast_to(weight[0:1, part], (8, LANES))
            pk = jnp.broadcast_to(packed[0:1, part], (8, LANES))
            hit = high == k
            w = jnp.where(hit, jnp.take_along_axis(wk, low, axis=1), w)
            p = jnp.where(hit, jnp.take_along_axis(pk, low, axis=1), p)
        first = p & 4095
        second = p >> 12
        other = jnp.where(first == lane + tile * LANES, second, first)
        away = other - cell_count
        place = jnp.zeros((8, LANES), jnp.int32)
        for k in range(6):
            inside = (away >= k * length) & (away < (k + 1) * length)
            place = jnp.where(inside, away - k * length + base[k], place)
        near = jnp.where(away < 0, other, cell_count + place)
        share = w / area_ref[0:1, here]
        share = jnp.where(row < 6, share, 0.0)
        total = jnp.sum(share, axis=0, keepdims=True)
        near_ref[:, here] = jnp.where(row < 6, near, -1)
        coef_ref[:, here] = jnp.where(row == 6, total, share)
    for k in range(6):
        rows = lax.broadcasted_iota(jnp.int32, (counts[k], length), 0)
        columns = lax.broadcasted_iota(jnp.int32, (counts[k], length), 1)
        ids = send_ref[k : k + 1, :].astype(jnp.float32)
        column = jnp.sum(jnp.where(rows == columns, ids, 0.0), axis=1, keepdims=True)
        cols_ref[base[k] : base[k] + counts[k], :] = jnp.broadcast_to(
            column, (counts[k], LANES)
        ).astype(jnp.int32)


def split(values):
    high = values.astype(jnp.bfloat16)
    low = (values - high.astype(jnp.float32)).astype(jnp.bfloat16)
    return high, low


def main_kernel(
    devices, length, field_ref, near_ref, coef_ref, cols_ref, out_ref,
    landed, flat, first, matrix, rim, triple, selector, outgoing, incoming,
    load_sem, send_sem, recv_sem,
):
    fields_n, levels_n, cell_count = field_ref.shape
    stride = up(levels_n, 8)
    chunk = flat.shape[0] // CHUNKS
    halo = rim.shape[0] // 3
    base, counts, used = slots(length)
    me = lax.axis_index("cells")
    targets = [lax.rem(me + (o + devices), devices) for o in OFFSETS]

    loads = [
        pltpu.make_async_copy(field_ref.at[f], landed.at[f], load_sem.at[f])
        for f in range(fields_n)
    ]
    for load in loads:
        load.start()

    barrier = pltpu.get_barrier_semaphore()
    for target in targets:
        pl.semaphore_signal(
            barrier, inc=1, device_id=(target,), device_id_type=pl.DeviceIdType.MESH
        )

    lane = lax.broadcasted_iota(jnp.int32, (used, LANES), 1)
    for tile in range(cell_count // LANES):
        hit = cols_ref[...] == lane + tile * LANES
        ones = jnp.where(hit, 1.0, 0.0).astype(jnp.bfloat16)
        selector[:, tile * LANES : (tile + 1) * LANES] = ones
        at = cell_count + tile * LANES
        selector[:, at : at + LANES] = ones
    for lap in range(2):
        for c in range(CHUNKS):
            incoming[lap, c, used:, :] = jnp.zeros((halo - used, chunk), jnp.float32)
    rows = flat.shape[0]
    end = fields_n * stride
    if rows > end:
        flat[end:, :] = jnp.zeros((rows - end, cell_count), jnp.float32)
    if stride > levels_n:
        for f in range(fields_n):
            at = (f + 1) * stride - 8
            flat[at : at + 8, :] = jnp.zeros((8, cell_count), jnp.float32)

    def spread(values, c):
        high, low = split(values)
        triple[c, :, :cell_count] = high
        triple[c, :, cell_count : 2 * cell_count] = low
        triple[c, :, 2 * cell_count :] = high

    def copies(lap, c):
        return [
            pltpu.make_async_remote_copy(
                src_ref=outgoing.at[lap, c, pl.ds(base[k], counts[k])],
                dst_ref=incoming.at[lap, c, pl.ds(base[k], counts[k])],
                send_sem=send_sem.at[lap, c, k],
                recv_sem=recv_sem.at[lap, c, k],
                device_id=(targets[k],),
                device_id_type=pl.DeviceIdType.MESH,
            )
            for k in (2, 3, 4, 5, 0, 1)
        ]

    def send(lap, c):
        outgoing[lap, c] = lax.dot_general(
            selector[...],
            triple[c, :, : 2 * cell_count],
            (((1,), (1,)), ((), ())),
            preferred_element_type=jnp.float32,
        )
        for copy in copies(lap, c):
            copy.start()

    def own(c):
        return jnp.dot(triple[c], matrix[...], preferred_element_type=jnp.float32)

    def outside(lap, c):
        for copy in copies(lap, c):
            copy.wait_recv()
        high, low = split(incoming[lap, c].T)
        lhs = jnp.concatenate([high, low, high], axis=1)
        return jnp.dot(lhs, rim[...], preferred_element_type=jnp.float32)

    loaded = 0
    for c in range(CHUNKS):
        need = min(fields_n, -(-((c + 1) * chunk) // stride))
        for f in range(loaded, need):
            loads[f].wait()
            flat[f * stride : f * stride + levels_n, :] = landed[f]
        loaded = max(loaded, need)
        spread(flat[c * chunk : (c + 1) * chunk, :], c)
        if c == 0:
            pl.semaphore_wait(barrier, len(targets))
        send(0, c)

    ids = lax.broadcasted_iota(jnp.int32, (LANES, LANES), 0)

    def entries(start, tile):
        here = slice(tile * LANES, (tile + 1) * LANES)
        block = jnp.zeros((LANES, LANES), jnp.float32)
        for j in range(6):
            hit = ids == near_ref[j : j + 1, here] - start
            block = jnp.where(hit, coef_ref[j : j + 1, here], block)
        return split(block)

    def fill(r, carry):
        start = pl.multiple_of(r * LANES, LANES)
        for tile in range(cell_count // LANES):
            here = slice(tile * LANES, (tile + 1) * LANES)
            high, low = entries(start, tile)
            matrix[pl.ds(start, LANES), here] = high
            matrix[pl.ds(start + cell_count, LANES), here] = high
            matrix[pl.ds(start + 2 * cell_count, LANES), here] = low
        return carry

    lax.fori_loop(0, cell_count // LANES, fill, 0)
    for r in range(halo // LANES):
        for tile in range(cell_count // LANES):
            here = slice(tile * LANES, (tile + 1) * LANES)
            high, low = entries(cell_count + r * LANES, tile)
            rim[r * LANES : (r + 1) * LANES, here] = high
            rim[halo + r * LANES : halo + (r + 1) * LANES, here] = high
            rim[2 * halo + r * LANES : 2 * halo + (r + 1) * LANES, here] = low

    for c in range(CHUNKS):
        part = slice(c * chunk, (c + 1) * chunk)
        first[part, :] = own(c) - flat[part, :] * coef_ref[6:7, :]
        result = first[part, :] + outside(0, c)
        first[part, :] = result
        spread(result, c)
        send(1, c)
    for c in range(CHUNKS):
        part = slice(c * chunk, (c + 1) * chunk)
        out_ref[part, :] = own(c) - first[part, :] * coef_ref[6:7, :]
        out_ref[part, :] = out_ref[part, :] + outside(1, c)
    for lap in range(2):
        for c in range(CHUNKS):
            for copy in copies(lap, c):
                copy.wait_send()


def shards(
    devices, field, cell_area, dv_edge, dc_edge, cells_on_edge, edges_on_cell, send_cells,
    level_coef,
):
    length = send_cells.shape[1]
    fields_n, levels_n, cell_count = field.shape
    edge_count = dv_edge.shape[0]
    _, _, used = slots(length)
    halo = up(used, LANES)
    stride = up(levels_n, 8)
    rows = up(fields_n * stride, CHUNKS * LANES)
    chunk = rows // CHUNKS
    vmem = pl.BlockSpec(memory_space=pltpu.VMEM)
    near, coef, cols = pl.pallas_call(
        prepare_kernel,
        out_shape=(
            jax.ShapeDtypeStruct((8, cell_count), jnp.int32),
            jax.ShapeDtypeStruct((8, cell_count), jnp.float32),
            jax.ShapeDtypeStruct((used, LANES), jnp.int32),
        ),
        in_specs=[vmem] * 6,
        out_specs=(vmem,) * 3,
        scratch_shapes=[
            pltpu.VMEM((1, up(edge_count, LANES)), jnp.float32),
            pltpu.VMEM((1, up(edge_count, LANES)), jnp.int32),
            pltpu.VMEM((8, cell_count), jnp.int32),
        ],
        compiler_params=pltpu.CompilerParams(vmem_limit_bytes=8 * 1024 * 1024),
        name="prepare",
    )(
        dv_edge.reshape(1, edge_count),
        dc_edge.reshape(1, edge_count),
        cells_on_edge,
        edges_on_cell,
        send_cells,
        cell_area.reshape(1, cell_count),
    )
    second = pl.pallas_call(
        functools.partial(main_kernel, devices, length),
        out_shape=jax.ShapeDtypeStruct((rows, cell_count), jnp.float32),
        in_specs=[pl.BlockSpec(memory_space=pl.ANY), vmem, vmem, vmem],
        out_specs=vmem,
        scratch_shapes=[
            pltpu.VMEM((fields_n, levels_n, cell_count), jnp.float32),
            pltpu.VMEM((rows, cell_count), jnp.float32),
            pltpu.VMEM((rows, cell_count), jnp.float32),
            pltpu.VMEM((3 * cell_count, cell_count), jnp.bfloat16),
            pltpu.VMEM((3 * halo, cell_count), jnp.bfloat16),
            pltpu.VMEM((CHUNKS, chunk, 3 * cell_count), jnp.bfloat16),
            pltpu.VMEM((used, 2 * cell_count), jnp.bfloat16),
            pltpu.VMEM((2, CHUNKS, used, chunk), jnp.float32),
            pltpu.VMEM((2, CHUNKS, halo, chunk), jnp.float32),
            pltpu.SemaphoreType.DMA((fields_n,)),
            pltpu.SemaphoreType.DMA((2, CHUNKS, 6)),
            pltpu.SemaphoreType.DMA((2, CHUNKS, 6)),
        ],
        compiler_params=pltpu.CompilerParams(
            collective_id=0, has_side_effects=True, vmem_limit_bytes=44 * 1024 * 1024
        ),
        name="diffuse",
    )(field, near, coef, cols)
    second = second[: fields_n * stride].reshape(fields_n, stride, cell_count)[:, :levels_n]
    return -level_coef[None, :, None] * second


def solution(mesh):
    return jax.shard_map(
        functools.partial(shards, mesh.shape["cells"]),
        mesh=mesh,
        in_specs=(
            P(None, None, "cells"),
            P("cells"),
            P("cells"),
            P("cells"),
            P(None, "cells"),
            P(None, "cells"),
            P(None, "cells"),
            P(),
        ),
        out_specs=P(None, None, "cells"),
        check_vma=False,
    )
```

```python
import functools

import jax
import jax.numpy as jnp
from jax import lax
from jax.experimental import pallas as pl
from jax.experimental.pallas import tpu as pltpu
from jax.sharding import PartitionSpec as P

CELLS_Y = 16
BLOCK_ROW = 16
OFFSETS = (1, -1, BLOCK_ROW, -BLOCK_ROW, BLOCK_ROW - 1, 1 - BLOCK_ROW)
LANES = 128
CHUNKS = 2


def up(value, step):
    return -(-value // step) * step


def slots(length):
    side = CELLS_Y
    counts = (side, side, length, length, 8, 8)
    order = (2, 3, 0, 1, 4, 5)
    base = [0] * 6
    at = 0
    for k in order:
        base[k] = at
        at += counts[k]
    return tuple(base), counts, at


def prepare_kernel(
    dv_hbm, dc_hbm, ends_hbm, edges_hbm, send_hbm, area_hbm, near_ref, coef_ref, cols_ref,
    weight, packed, index, dv_ref, dc_ref, ends_ref, edges_ref, send_ref, area_ref, sems,
):
    pairs = (
        (dv_hbm, dv_ref), (dc_hbm, dc_ref), (ends_hbm, ends_ref), (edges_hbm, edges_ref),
        (send_hbm, send_ref), (area_hbm, area_ref),
    )
    loads = [pltpu.make_async_copy(a, b, sems.at[i]) for i, (a, b) in enumerate(pairs)]
    for load in loads:
        load.start()
    edge_count = ends_ref.shape[1]
    cell_count = edges_ref.shape[1]
    length = send_ref.shape[1]
    base, counts, _ = slots(length)
    tables = weight.shape[1] // LANES
    weight[...] = jnp.zeros_like(weight)
    packed[...] = jnp.zeros_like(packed)
    index[...] = jnp.zeros_like(index)
    for load in loads:
        load.wait()
    for k in range(tables):
        part = slice(k * LANES, min((k + 1) * LANES, edge_count))
        weight[0, part] = dv_ref[part] / dc_ref[part]
    packed[:, :edge_count] = ends_ref[0:1, :] + ends_ref[1:2, :] * 4096
    index[0:6, :] = edges_ref[...]
    row = lax.broadcasted_iota(jnp.int32, (8, LANES), 0)
    lane = lax.broadcasted_iota(jnp.int32, (8, LANES), 1)
    for tile in range(cell_count // LANES):
        here = slice(tile * LANES, (tile + 1) * LANES)
        wanted = index[:, here]
        high = wanted >> 7
        low = wanted & 127
        w = jnp.zeros((8, LANES), jnp.float32)
        p = jnp.zeros((8, LANES), jnp.int32)
        for k in range(tables):
            part = slice(k * LANES, (k + 1) * LANES)
            wk = jnp.broadcast_to(weight[0:1, part], (8, LANES))
            pk = jnp.broadcast_to(packed[0:1, part], (8, LANES))
            hit = high == k
            w = jnp.where(hit, jnp.take_along_axis(wk, low, axis=1), w)
            p = jnp.where(hit, jnp.take_along_axis(pk, low, axis=1), p)
        first = p & 4095
        second = p >> 12
        other = jnp.where(first == lane + tile * LANES, second, first)
        away = other - cell_count
        place = jnp.zeros((8, LANES), jnp.int32)
        for k in range(6):
            inside = (away >= k * length) & (away < (k + 1) * length)
            place = jnp.where(inside, away - k * length + base[k], place)
        near = jnp.where(away < 0, other, cell_count + place)
        share = w / jnp.broadcast_to(area_ref[here], (8, LANES))
        share = jnp.where(row < 6, share, 0.0)
        total = jnp.sum(share, axis=0, keepdims=True)
        near_ref[:, here] = jnp.where(row < 6, near, -1)
        coef_ref[:, here] = jnp.where(row == 6, total, share)
    for k in range(6):
        rows = lax.broadcasted_iota(jnp.int32, (counts[k], length), 0)
        columns = lax.broadcasted_iota(jnp.int32, (counts[k], length), 1)
        ids = send_ref[k : k + 1, :].astype(jnp.float32)
        column = jnp.sum(jnp.where(rows == columns, ids, 0.0), axis=1, keepdims=True)
        cols_ref[base[k] : base[k] + counts[k], :] = jnp.broadcast_to(
            column, (counts[k], LANES)
        ).astype(jnp.int32)


def split(values):
    high = values.astype(jnp.bfloat16)
    low = (values - high.astype(jnp.float32)).astype(jnp.bfloat16)
    return high, low


def main_kernel(
    devices, length, field_ref, near_ref, coef_ref, cols_ref, out_ref,
    landed, flat, first, matrix, rim, triple, selector, outgoing, incoming,
    load_sem, send_sem, recv_sem,
):
    fields_n, levels_n, cell_count = field_ref.shape
    stride = up(levels_n, 8)
    chunk = flat.shape[0] // CHUNKS
    halo = rim.shape[0] // 3
    base, counts, used = slots(length)
    me = lax.axis_index("cells")
    targets = [lax.rem(me + (o + devices), devices) for o in OFFSETS]

    loads = [
        pltpu.make_async_copy(field_ref.at[f], landed.at[f], load_sem.at[f])
        for f in range(fields_n)
    ]
    for load in loads:
        load.start()

    barrier = pltpu.get_barrier_semaphore()
    for target in targets:
        pl.semaphore_signal(
            barrier, inc=1, device_id=(target,), device_id_type=pl.DeviceIdType.MESH
        )

    lane = lax.broadcasted_iota(jnp.int32, (used, LANES), 1)
    for tile in range(cell_count // LANES):
        hit = cols_ref[...] == lane + tile * LANES
        ones = jnp.where(hit, 1.0, 0.0).astype(jnp.bfloat16)
        selector[:, tile * LANES : (tile + 1) * LANES] = ones
        at = cell_count + tile * LANES
        selector[:, at : at + LANES] = ones
    for lap in range(2):
        for c in range(CHUNKS):
            incoming[lap, c, used:, :] = jnp.zeros((halo - used, chunk), jnp.float32)
    rows = flat.shape[0]
    end = fields_n * stride
    if rows > end:
        flat[end:, :] = jnp.zeros((rows - end, cell_count), jnp.float32)
    if stride > levels_n:
        for f in range(fields_n):
            at = (f + 1) * stride - 8
            flat[at : at + 8, :] = jnp.zeros((8, cell_count), jnp.float32)

    def spread(values, c):
        high, low = split(values)
        triple[c, :, :cell_count] = high
        triple[c, :, cell_count : 2 * cell_count] = low
        triple[c, :, 2 * cell_count :] = high

    def copies(lap, c):
        return [
            pltpu.make_async_remote_copy(
                src_ref=outgoing.at[lap, c, pl.ds(base[k], counts[k])],
                dst_ref=incoming.at[lap, c, pl.ds(base[k], counts[k])],
                send_sem=send_sem.at[lap, c, k],
                recv_sem=recv_sem.at[lap, c, k],
                device_id=(targets[k],),
                device_id_type=pl.DeviceIdType.MESH,
            )
            for k in (2, 3, 4, 5, 0, 1)
        ]

    def send(lap, c):
        outgoing[lap, c] = lax.dot_general(
            selector[...],
            triple[c, :, : 2 * cell_count],
            (((1,), (1,)), ((), ())),
            preferred_element_type=jnp.float32,
        )
        for copy in copies(lap, c):
            copy.start()

    def own(c):
        return jnp.dot(triple[c], matrix[...], preferred_element_type=jnp.float32)

    def outside(lap, c):
        for copy in copies(lap, c):
            copy.wait_recv()
        high, low = split(incoming[lap, c].T)
        lhs = jnp.concatenate([high, low, high], axis=1)
        return jnp.dot(lhs, rim[...], preferred_element_type=jnp.float32)

    loaded = 0
    for c in range(CHUNKS):
        need = min(fields_n, -(-((c + 1) * chunk) // stride))
        for f in range(loaded, need):
            loads[f].wait()
            flat[f * stride : f * stride + levels_n, :] = landed[f]
        loaded = max(loaded, need)
        spread(flat[c * chunk : (c + 1) * chunk, :], c)
        if c == 0:
            pl.semaphore_wait(barrier, len(targets))
        send(0, c)

    ids = lax.broadcasted_iota(jnp.int32, (LANES, LANES), 0)

    def entries(start, tile):
        here = slice(tile * LANES, (tile + 1) * LANES)
        block = jnp.zeros((LANES, LANES), jnp.float32)
        for j in range(6):
            hit = ids == near_ref[j : j + 1, here] - start
            block = jnp.where(hit, coef_ref[j : j + 1, here], block)
        return split(block)

    def fill(r, carry):
        start = pl.multiple_of(r * LANES, LANES)
        for tile in range(cell_count // LANES):
            here = slice(tile * LANES, (tile + 1) * LANES)
            high, low = entries(start, tile)
            matrix[pl.ds(start, LANES), here] = high
            matrix[pl.ds(start + cell_count, LANES), here] = high
            matrix[pl.ds(start + 2 * cell_count, LANES), here] = low
        return carry

    lax.fori_loop(0, cell_count // LANES, fill, 0)
    for r in range(halo // LANES):
        for tile in range(cell_count // LANES):
            here = slice(tile * LANES, (tile + 1) * LANES)
            high, low = entries(cell_count + r * LANES, tile)
            rim[r * LANES : (r + 1) * LANES, here] = high
            rim[halo + r * LANES : halo + (r + 1) * LANES, here] = high
            rim[2 * halo + r * LANES : 2 * halo + (r + 1) * LANES, here] = low

    for c in range(CHUNKS):
        part = slice(c * chunk, (c + 1) * chunk)
        first[part, :] = own(c) - flat[part, :] * coef_ref[6:7, :]
        result = first[part, :] + outside(0, c)
        first[part, :] = result
        spread(result, c)
        send(1, c)
    for c in range(CHUNKS):
        part = slice(c * chunk, (c + 1) * chunk)
        out_ref[part, :] = own(c) - first[part, :] * coef_ref[6:7, :]
        out_ref[part, :] = out_ref[part, :] + outside(1, c)
    for lap in range(2):
        for c in range(CHUNKS):
            for copy in copies(lap, c):
                copy.wait_send()


def shards(
    devices, field, cell_area, dv_edge, dc_edge, cells_on_edge, edges_on_cell, send_cells,
    level_coef,
):
    length = send_cells.shape[1]
    fields_n, levels_n, cell_count = field.shape
    edge_count = dv_edge.shape[0]
    _, _, used = slots(length)
    halo = up(used, LANES)
    stride = up(levels_n, 8)
    rows = up(fields_n * stride, CHUNKS * LANES)
    chunk = rows // CHUNKS
    vmem = pl.BlockSpec(memory_space=pltpu.VMEM)
    hbm = pl.BlockSpec(memory_space=pltpu.HBM)
    near, coef, cols = pl.pallas_call(
        prepare_kernel,
        out_shape=(
            jax.ShapeDtypeStruct((8, cell_count), jnp.int32),
            jax.ShapeDtypeStruct((8, cell_count), jnp.float32),
            jax.ShapeDtypeStruct((used, LANES), jnp.int32),
        ),
        in_specs=[hbm] * 6,
        out_specs=(vmem,) * 3,
        scratch_shapes=[
            pltpu.VMEM((1, up(edge_count, LANES)), jnp.float32),
            pltpu.VMEM((1, up(edge_count, LANES)), jnp.int32),
            pltpu.VMEM((8, cell_count), jnp.int32),
            pltpu.VMEM(dv_edge.shape, jnp.float32),
            pltpu.VMEM(dc_edge.shape, jnp.float32),
            pltpu.VMEM(cells_on_edge.shape, jnp.int32),
            pltpu.VMEM(edges_on_cell.shape, jnp.int32),
            pltpu.VMEM(send_cells.shape, jnp.int32),
            pltpu.VMEM(cell_area.shape, jnp.float32),
            pltpu.SemaphoreType.DMA((6,)),
        ],
        compiler_params=pltpu.CompilerParams(vmem_limit_bytes=67043328),
        name="prepare",
    )(
        dv_edge,
        dc_edge,
        cells_on_edge,
        edges_on_cell,
        send_cells,
        cell_area,
    )
    second = pl.pallas_call(
        functools.partial(main_kernel, devices, length),
        out_shape=jax.ShapeDtypeStruct((rows, cell_count), jnp.float32),
        in_specs=[hbm, vmem, vmem, vmem],
        out_specs=vmem,
        scratch_shapes=[
            pltpu.VMEM((fields_n, levels_n, cell_count), jnp.float32),
            pltpu.VMEM((rows, cell_count), jnp.float32),
            pltpu.VMEM((rows, cell_count), jnp.float32),
            pltpu.VMEM((3 * cell_count, cell_count), jnp.bfloat16),
            pltpu.VMEM((3 * halo, cell_count), jnp.bfloat16),
            pltpu.VMEM((CHUNKS, chunk, 3 * cell_count), jnp.bfloat16),
            pltpu.VMEM((used, 2 * cell_count), jnp.bfloat16),
            pltpu.VMEM((2, CHUNKS, used, chunk), jnp.float32),
            pltpu.VMEM((2, CHUNKS, halo, chunk), jnp.float32),
            pltpu.SemaphoreType.DMA((fields_n,)),
            pltpu.SemaphoreType.DMA((2, CHUNKS, 6)),
            pltpu.SemaphoreType.DMA((2, CHUNKS, 6)),
        ],
        compiler_params=pltpu.CompilerParams(
            collective_id=0, has_side_effects=True, vmem_limit_bytes=44 * 1024 * 1024
        ),
        name="diffuse",
    )(field, near, coef, cols)
    second = second[: fields_n * stride].reshape(fields_n, stride, cell_count)[:, :levels_n]
    return -level_coef[None, :, None] * second


def solution(mesh):
    return jax.shard_map(
        functools.partial(shards, mesh.shape["cells"]),
        mesh=mesh,
        in_specs=(
            P(None, None, "cells"),
            P("cells"),
            P("cells"),
            P("cells"),
            P(None, "cells"),
            P(None, "cells"),
            P(None, "cells"),
            P(),
        ),
        out_specs=P(None, None, "cells"),
        check_vma=False,
    )
```
